32 devices in a mesh: grid: 16 (over z, x, core), band: 2 (over y).
Axes of the slice: x: 2, y: 2, z: 4, core: 2. Of those that a mesh axis runs over, the one named last changes fastest.
Arguments:
- states: float32 [4096, 256], P('grid', 'band'), may hold values from -6 to 6
- potential: float32 [4096], P('grid'), may hold values from -3 to 0
- bounds: float32 [3], replicated, may hold values from -9 to 26, as said below
- point_count: int32 [16], P('grid'), may hold values from 128 to 256, as said below
- send_rows: int32 [16, 6, 64], P('grid'), may hold values from 0 to 256, as said below
- stencil_table: int32 [36, 4096], P(None, 'grid'), may hold values from 0 to 640, as said below
Outputs:
- filtered: float32 [4096, 256], P('grid', 'band')
- margin: float32 [256, 256], P(('grid', 'band'))
The draws below stay inside these ranges and needn't reach their ends.
Inputs may be any that keep to these rules, and one draw needn't show every extreme that they name: `point_count`: one partition has exactly 256 live points in every draw; rows at or past a partition's count are padding. send_rows[g, k, j] is the row of partition g sent as row j of its block to partition g + o_k (o_k as in the reference program). A block has a length from half of 64 to 64: below it the entries are live rows of g, from it on they are 256; some block is full in every draw. Blocks to partitions that do not exist hold only 256. stencil_table[s, g * 256 + r] indexes E_g: values below 256 are live rows of partition g, 256 is the zero row, 257 + k * 64 + j is row j of the block from partition g - o_k, named only when that partition exists. Padding rows hold only 256; rows r below 160 name no block. bounds holds lower, cutoff and upper in this order: lower between -9 and -5, cutoff between -1.5 and 1.5, upper between 21 and 26.
All inputs are finite; a program needn't handle non-finite values.
Results may differ from the reference program's by a relative error of at most 0.0018.
Values may be sent and summed in bfloat16 or wider, within the bound.
A program may use at most 64 MiB of HBM per device.

```python
import jax
import jax.numpy as jnp
from jax import lax

P_DEV = 256
HALO = 64
REACH = 3
SPAN = 6
DEGREE = 3
STENCIL = 36
INNER = 160
POINTS = 4096
BANDS = 256
N_GRID = 16


def partition_sizes(key):
    sizes = jax.random.randint(jax.random.fold_in(key, 11), (N_GRID,), P_DEV // 2, P_DEV + 1)
    fullest = jax.random.randint(jax.random.fold_in(key, 12), (), 0, N_GRID)
    return jnp.where(jnp.arange(N_GRID) == fullest, P_DEV, sizes).astype(jnp.int32)


def slot_offsets():
    slots = jnp.arange(2 * REACH)
    return jnp.where(slots < REACH, slots - REACH, slots - REACH + 1)


def draw_point_count(key, part):
    return partition_sizes(key)


def draw_send_rows(key, part):
    sizes = partition_sizes(key)
    lengths = jax.random.randint(jax.random.fold_in(key, 21), (N_GRID, 2 * REACH), HALO // 2, HALO + 1)
    full_source = jax.random.randint(jax.random.fold_in(key, 22), (), 0, N_GRID - REACH)
    full_slot = jax.random.randint(jax.random.fold_in(key, 23), (), REACH, 2 * REACH)
    partitions = jnp.arange(N_GRID)[:, None]
    slots = jnp.arange(2 * REACH)[None, :]
    lengths = jnp.where(jnp.logical_and(partitions == full_source, slots == full_slot), HALO, lengths)
    target = partitions + slot_offsets()[None, :]
    exists = jnp.logical_and(target >= 0, target < N_GRID)
    picks = jax.random.randint(jax.random.fold_in(key, 24), (N_GRID, 2 * REACH, HALO), 0, 1 << 30) % sizes[:, None, None]
    positions = jnp.arange(HALO)[None, None, :]
    used = jnp.logical_and(positions < lengths[:, :, None], exists[:, :, None])
    return jnp.where(used, picks, P_DEV).astype(jnp.int32)


def draw_stencil_table(key, part):
    sizes = partition_sizes(key)
    shaped = (STENCIL, N_GRID, P_DEV)
    kinds = jax.random.randint(jax.random.fold_in(key, 31), shaped, 0, 20)
    local_pick = jax.random.randint(jax.random.fold_in(key, 32), shaped, 0, 1 << 30) % sizes[None, :, None]
    ghost_slot = jax.random.randint(jax.random.fold_in(key, 33), shaped, 0, 2 * REACH)
    ghost_row = jax.random.randint(jax.random.fold_in(key, 34), shaped, 0, HALO)
    partitions = jnp.arange(N_GRID)[None, :, None]
    source = partitions - slot_offsets()[ghost_slot]
    exists = jnp.logical_and(source >= 0, source < N_GRID)
    row_index = jnp.arange(P_DEV)[None, None, :]
    ghost_index = P_DEV + 1 + ghost_slot * HALO + ghost_row
    use_ghost = jnp.logical_and(jnp.logical_and(kinds >= 14, kinds < 19), row_index >= INNER)
    chosen = jnp.where(jnp.logical_and(use_ghost, exists), ghost_index, local_pick)
    chosen = jnp.where(jnp.logical_and(use_ghost, jnp.logical_not(exists)), P_DEV, chosen)
    chosen = jnp.where(jnp.logical_or(kinds >= 19, row_index >= sizes[None, :, None]), P_DEV, chosen)
    return chosen.reshape(STENCIL, N_GRID * P_DEV).astype(jnp.int32)


def draw_bounds(key, part):
    lower_bound = jax.random.uniform(jax.random.fold_in(key, 41), (), jnp.float32, -8.0, -6.0)
    cutoff = jax.random.uniform(jax.random.fold_in(key, 42), (), jnp.float32, -1.0, 1.0)
    upper_bound = jax.random.uniform(jax.random.fold_in(key, 43), (), jnp.float32, 22.0, 25.0)
    return jnp.stack([lower_bound, cutoff, upper_bound]).astype(jnp.float32)


def level_of(stream_key, extent, shards, low, largest):
    loudness, own = 1.0, jax.random.fold_in(stream_key, 6)
    for axis_at, blocks in shards:
        steps = jnp.exp(jax.random.uniform(jax.random.fold_in(own, axis_at), (blocks,), jnp.float32, low / len(shards), largest / len(shards)))
        loudness = loudness * jnp.repeat(steps, extent[axis_at] // blocks).reshape([-1 if axis == axis_at else 1 for axis in range(len(extent))])
    return loudness


def scatter_about(stream_key, extent, scale, limit, shards=(), held_as=jnp.bfloat16):
    gain = level_of(stream_key, extent, shards, -0.22, 0.18) if shards else 1.0
    values = jax.random.normal(stream_key, extent, jnp.float32) * scale * gain
    return jnp.minimum(jnp.maximum(values, -limit), limit).astype(held_as)


def setup_inputs(seed: int = 0) -> dict:
    streams_of = jax.random.split(jax.random.key(seed), 7)
    states = scatter_about(streams_of[0], (POINTS, BANDS), 1.0, 6.0, ((0, 16), (1, 2)), jnp.float32)
    potential = jnp.clip(-3.0 + 3.0 * jax.random.uniform(streams_of[1], (POINTS,), jnp.float32) ** level_of(streams_of[1], (POINTS,), ((0, 16),), -0.2, 0.2), -3.0, 0.0)
    bounds = draw_bounds(jax.random.fold_in(streams_of[6], 71), 0)
    point_count = draw_point_count(jax.random.fold_in(streams_of[6], 71), 0)
    send_rows = draw_send_rows(jax.random.fold_in(streams_of[6], 71), 0)
    stencil_table = draw_stencil_table(jax.random.fold_in(streams_of[6], 71), 0)
    return {"states": states, "potential": potential, "bounds": bounds, "point_count": point_count, "send_rows": send_rows, "stencil_table": stencil_table}


DIFFERENCE_WEIGHTS = (-5369.0 / 1800.0, 12.0 / 7.0, -15.0 / 56.0, 10.0 / 189.0, -1.0 / 112.0, 2.0 / 1925.0, -1.0 / 16632.0)
KINETIC_SCALE = 0.5 / 0.49
CENTRE_WEIGHT = -3.0 * KINETIC_SCALE * DIFFERENCE_WEIGHTS[0]


def apply_stencil(extended, local_table, fields, potentials):
    result = (potentials + CENTRE_WEIGHT)[:, None] * fields
    for neighbour in range(local_table.shape[0]):
        weight = -KINETIC_SCALE * DIFFERENCE_WEIGHTS[neighbour % SPAN + 1]
        result = result + weight * jnp.take(extended, local_table[neighbour], axis=0)
    return result


def apply_operator(fields, potentials, send_rows, stencil_table):
    grid_count, row_count, band_total = fields.shape
    half_slots = send_rows.shape[1] // 2
    zero_row = jnp.zeros((1, band_total), jnp.float32)

    def partition_image(partition):
        pieces = [fields[partition], zero_row]
        for slot_index in range(2 * half_slots):
            offset = slot_index - half_slots if slot_index < half_slots else slot_index - half_slots + 1
            source = partition - offset
            inside = jnp.logical_and(source >= 0, source < grid_count)
            clipped = jnp.clip(source, 0, grid_count - 1)
            source_rows = jnp.concatenate([fields[clipped], zero_row], axis=0)
            outgoing = jnp.take(source_rows, send_rows[clipped, slot_index], axis=0)
            pieces.append(jnp.where(inside, outgoing, 0.0))
        extended = jnp.concatenate(pieces, axis=0)
        local_table = lax.dynamic_slice_in_dim(stencil_table, partition * row_count, row_count, 1)
        return apply_stencil(extended, local_table, fields[partition], potentials[partition])

    return lax.map(partition_image, jnp.arange(grid_count, dtype=jnp.int32))


def reference(states, potential, bounds, point_count, send_rows, stencil_table):
    fields = states.reshape(N_GRID, P_DEV, BANDS)
    potentials = potential.reshape(N_GRID, P_DEV)
    live_rows = jnp.arange(P_DEV, dtype=jnp.int32)[None, :] < point_count[:, None]
    previous = jnp.where(live_rows[:, :, None], fields, 0.0)
    lower_bound = bounds[0]
    cutoff = bounds[1]
    upper_bound = bounds[2]
    half_width = (upper_bound - cutoff) / 2.0
    middle = (upper_bound + cutoff) / 2.0
    sigma_now = half_width / (lower_bound - middle)
    twice_inverse = 2.0 / sigma_now
    applied = apply_operator(previous, potentials, send_rows, stencil_table)
    current = (applied - middle * previous) * (sigma_now / half_width)
    for degree_index in range(DEGREE - 1):
        sigma_next = 1.0 / (twice_inverse - sigma_now)
        applied = apply_operator(current, potentials, send_rows, stencil_table)
        following = (applied - middle * current) * (2.0 * sigma_next / half_width) - (sigma_now * sigma_next) * previous
        previous = current
        current = following
        sigma_now = sigma_next
    filtered = current.reshape(POINTS, BANDS)
    rounded = filtered.astype(jnp.bfloat16)
    margin = jnp.dot(rounded.T, rounded, preferred_element_type=jnp.float32) * (1.0 / POINTS)
    return filtered, margin
```

```python
import functools

import jax
import jax.numpy as jnp
from jax import lax
from jax.experimental import pallas as pl
from jax.experimental.pallas import tpu as pltpu
from jax.sharding import PartitionSpec as P

SPAN = 6
DEGREE = 3
INNER = 160

DIFFERENCE_WEIGHTS = (
    -5369.0 / 1800.0,
    12.0 / 7.0,
    -15.0 / 56.0,
    10.0 / 189.0,
    -1.0 / 112.0,
    2.0 / 1925.0,
    -1.0 / 16632.0,
)
KINETIC_SCALE = 0.5 / 0.49
CENTRE_WEIGHT = -3.0 * KINETIC_SCALE * DIFFERENCE_WEIGHTS[0]

MESH = pl.DeviceIdType.MESH
F32 = jnp.float32
BF16 = jnp.bfloat16


def dot(a, b):
    return jnp.dot(a, b, preferred_element_type=F32)


def gram(x):
    return lax.dot_general(x, x, (((0,), (0,)), ((), ())), preferred_element_type=F32)


def halves(x):
    high = x.astype(BF16)
    return high, (x - high.astype(F32)).astype(BF16)


def offset_of(slot, reach):
    return slot - reach if slot < reach else slot - reach + 1


def kernel(
    n_grid, n_band, bounds, count, states, potential, send_rows, table, filtered, margin,
    table_pad, send_pad, picks, near_hi, near_lo, far_hi, far_lo, out_box, in_box, bands, total,
    share_out, share_in, halo_sent, halo_got, band_sent, band_got, share_sent, share_got,
):
    rows, width = states.shape
    slots, halo = send_rows.shape[1:]
    reach = slots // 2
    stencil = table.shape[0]
    outer = rows - INNER
    per = margin.shape[0]
    g = lax.axis_index("grid")
    b = lax.axis_index("band")

    in_box[...] = jnp.zeros_like(in_box)
    barrier = pltpu.get_barrier_semaphore()
    for d in range(1, n_grid):
        pl.semaphore_signal(barrier, inc=1, device_id={"grid": lax.rem(g + d, n_grid)}, device_id_type=MESH)
    for d in range(1, n_band):
        pl.semaphore_signal(barrier, inc=1, device_id={"band": lax.rem(b + d, n_band)}, device_id_type=MESH)

    send_pad[...] = jnp.full(send_pad.shape, -1.0, F32)
    send_pad[:slots, :halo] = send_rows[0].astype(F32)
    send_columns = send_pad[...].T
    lanes = lax.broadcasted_iota(jnp.int32, (halo, rows), 1).astype(F32)
    for k in range(slots):
        hit = send_columns[:halo, k : k + 1] == lanes
        picks[k * halo : (k + 1) * halo, :] = jnp.where(hit, 1.0, 0.0).astype(BF16)

    def halo_copy(i, k, target):
        return pltpu.make_async_remote_copy(
            src_ref=out_box.at[i, k],
            dst_ref=in_box.at[i, k],
            send_sem=halo_sent.at[i, k],
            recv_sem=halo_got.at[i, k],
            device_id={"grid": target},
            device_id_type=MESH,
        )

    def send_halo(i, field):
        out_box[i] = dot(picks[...], field.astype(BF16)).astype(BF16).reshape(slots, halo, width)
        if i == 0:
            pl.semaphore_wait(barrier, n_grid - 1 + n_band - 1)
        for k in range(slots):
            target = g + offset_of(k, reach)

            @pl.when(jnp.logical_and(target >= 0, target < n_grid))
            def _():
                halo_copy(i, k, target).start()

    def wait_halo(i):
        for k in range(slots):
            source = g - offset_of(k, reach)

            @pl.when(jnp.logical_and(source >= 0, source < n_grid))
            def _():
                halo_copy(i, k, g).wait_recv()

    live = lax.broadcasted_iota(jnp.int32, (rows, width), 0) < count[0]
    previous = jnp.zeros((rows, width), F32)
    current = jnp.where(live, states[...], 0.0)
    send_halo(0, current)

    table_pad[...] = jnp.zeros_like(table_pad)
    table_pad[:stencil, :] = table[...].astype(F32)
    table_pad[stencil : stencil + 1, :] = potential[...]
    columns = table_pad[...].T
    weights = [-KINETIC_SCALE * DIFFERENCE_WEIGHTS[s % SPAN + 1] for s in range(stencil)]

    def weigh(first, size, start, extent):
        ids = (lax.broadcasted_iota(jnp.int32, (size, extent), 1) + start).astype(F32)
        acc = jnp.zeros((size, extent), F32)
        for s in range(stencil):
            acc = acc + jnp.where(columns[first : first + size, s : s + 1] == ids, weights[s], 0.0)
        return halves(acc)

    chunk = 32
    for first in range(0, rows, chunk):
        near_hi[first : first + chunk, :], near_lo[first : first + chunk, :] = weigh(first, chunk, 0, rows)
    for first in range(INNER, rows, chunk):
        at = slice(first - INNER, first - INNER + chunk)
        far_hi[at, :], far_lo[at, :] = weigh(first, chunk, rows + 1, slots * halo)

    def spread(value):
        return jnp.full((8, width), value, F32)

    lower, cutoff, upper = spread(bounds[0]), spread(bounds[1]), spread(bounds[2])
    half_width = (upper - cutoff) / 2.0
    middle = (upper + cutoff) / 2.0
    sigma = half_width / (lower - middle)
    twice_inverse = 2.0 / sigma
    diagonal = columns[:, stencil : stencil + 1] + CENTRE_WEIGHT - middle[:1, :]

    def near(field):
        high, low = halves(field)
        a = near_hi[...]
        return diagonal * field + (dot(a, high) + (dot(a, low) + dot(near_lo[...], high)))

    def far(i):
        box = in_box[i].reshape(slots * halo, width)
        return dot(far_hi[...], box) + dot(far_lo[...], box)

    gain = sigma / half_width
    back = jnp.zeros_like(sigma)
    for i in range(DEGREE):
        own = near(current)
        base = own * gain[:1, :] - back[:1, :] * previous
        if i < DEGREE - 1:
            wait_halo(i)
            outer_rows = base[INNER:] + far(i) * gain[:1, :]
            previous, current = current, jnp.concatenate([base[:INNER], outer_rows], axis=0)
            send_halo(i + 1, current)
            sigma_next = 1.0 / (twice_inverse - sigma)
            gain = 2.0 * sigma_next / half_width
            back = sigma * sigma_next
            sigma = sigma_next

    def band_copy(part, d):
        at = pl.ds(0, INNER) if part == 0 else pl.ds(INNER, outer)
        place = bands.at[b, at]
        return pltpu.make_async_remote_copy(
            src_ref=place,
            dst_ref=place,
            send_sem=band_sent.at[part, d - 1],
            recv_sem=band_got.at[part, d - 1],
            device_id={"band": lax.rem(b + d, n_band)},
            device_id_type=MESH,
        )

    def every_band(at):
        return jnp.concatenate([bands[j, at, :] for j in range(n_band)], axis=1)

    top, bottom = slice(0, INNER), slice(INNER, rows)
    filtered[top, :] = base[top]
    bands[b, top, :] = base[top].astype(BF16)
    for d in range(1, n_band):
        band_copy(0, d).start()
    for d in range(1, n_band):
        band_copy(0, d).wait_recv()
    total[...] = gram(every_band(top))
    wait_halo(DEGREE - 1)
    last = base[bottom] + far(DEGREE - 1) * gain[:1, :]
    bands[b, bottom, :] = last.astype(BF16)
    for d in range(1, n_band):
        band_copy(1, d).start()
    filtered[bottom, :] = last
    for d in range(1, n_band):
        band_copy(1, d).wait_recv()
    total[...] += gram(every_band(bottom))

    def share_copy(d):
        return pltpu.make_async_remote_copy(
            src_ref=share_out.at[d - 1],
            dst_ref=share_in.at[d - 1],
            send_sem=share_sent.at[d - 1],
            recv_sem=share_got.at[d - 1],
            device_id={"grid": lax.rem(g + d, n_grid)},
            device_id_type=MESH,
        )

    def share_of(owner):
        if per % 8 == 0:
            return total[pl.ds(pl.multiple_of((owner * n_band + b) * per, per), per), :]
        group = total[pl.ds(pl.multiple_of(owner * n_band * per, n_band * per), n_band * per), :]
        chosen = group[:per]
        for j in range(1, n_band):
            chosen = jnp.where(b == j, group[j * per : (j + 1) * per], chosen)
        return chosen

    for d in range(1, n_grid):
        share_out[d - 1] = share_of(lax.rem(g + d, n_grid)).astype(BF16)
    for d in range(1, n_grid):
        share_copy(d).start()
    result = share_of(g)
    for d in range(1, n_grid):
        share_copy(d).wait_recv()
    for d in range(1, n_grid):
        result = result + share_in[d - 1].astype(F32)
    margin[...] = result * (1.0 / (n_grid * rows))

    for i in range(DEGREE):
        for k in range(slots):
            target = g + offset_of(k, reach)

            @pl.when(jnp.logical_and(target >= 0, target < n_grid))
            def _():
                halo_copy(i, k, target).wait_send()

    for d in range(1, n_band):
        band_copy(0, d).wait_send()
        band_copy(1, d).wait_send()
    for d in range(1, n_grid):
        share_copy(d).wait_send()


def on_device(n_grid, n_band, states, potential, bounds, point_count, send_rows, stencil_table):
    rows, width = states.shape
    slots, halo = send_rows.shape[1:]
    total_bands = width * n_band
    per = total_bands // (n_grid * n_band)
    vmem = pl.BlockSpec(memory_space=pltpu.VMEM)
    smem = pl.BlockSpec(memory_space=pltpu.SMEM)
    dma = pltpu.SemaphoreType.DMA
    return pl.pallas_call(
        functools.partial(kernel, n_grid, n_band),
        out_shape=(
            jax.ShapeDtypeStruct((rows, width), F32),
            jax.ShapeDtypeStruct((per, total_bands), F32),
        ),
        in_specs=[smem, smem, vmem, vmem, vmem, vmem],
        out_specs=(vmem, vmem),
        scratch_shapes=[
            pltpu.VMEM((128, rows), F32),
            pltpu.VMEM((128, 128), F32),
            pltpu.VMEM((slots * halo, rows), BF16),
            pltpu.VMEM((rows, rows), BF16),
            pltpu.VMEM((rows, rows), BF16),
            pltpu.VMEM((rows - INNER, slots * halo), BF16),
            pltpu.VMEM((rows - INNER, slots * halo), BF16),
            pltpu.VMEM((DEGREE, slots, halo, width), BF16),
            pltpu.VMEM((DEGREE, slots, halo, width), BF16),
            pltpu.VMEM((n_band, rows, width), BF16),
            pltpu.VMEM((total_bands, total_bands), F32),
            pltpu.VMEM((n_grid - 1, per, total_bands), BF16),
            pltpu.VMEM((n_grid - 1, per, total_bands), BF16),
            dma((DEGREE, slots)),
            dma((DEGREE, slots)),
            dma((2, n_band - 1)),
            dma((2, n_band - 1)),
            dma((n_grid - 1,)),
            dma((n_grid - 1,)),
        ],
        compiler_params=pltpu.CompilerParams(collective_id=0, has_side_effects=True),
    )(bounds, point_count, states, potential.reshape(1, rows), send_rows, stencil_table)


def solution(mesh):
    placed = (P("grid", "band"), P("grid"), P(), P("grid"), P("grid", None, None), P(None, "grid"))
    return jax.shard_map(
        functools.partial(on_device, mesh.shape["grid"], mesh.shape["band"]),
        mesh=mesh,
        in_specs=placed,
        out_specs=(P("grid", "band"), P(("grid", "band"), None)),
        check_vma=False,
    )
```

```python
import functools

import jax
import jax.numpy as jnp
from jax import lax
from jax.experimental import pallas as pl
from jax.experimental.pallas import tpu as pltpu
from jax.sharding import PartitionSpec as P

SPAN = 6
DEGREE = 3
INNER = 160

DIFFERENCE_WEIGHTS = (
    -5369.0 / 1800.0,
    12.0 / 7.0,
    -15.0 / 56.0,
    10.0 / 189.0,
    -1.0 / 112.0,
    2.0 / 1925.0,
    -1.0 / 16632.0,
)
KINETIC_SCALE = 0.5 / 0.49
CENTRE_WEIGHT = -3.0 * KINETIC_SCALE * DIFFERENCE_WEIGHTS[0]

MESH = pl.DeviceIdType.MESH
F32 = jnp.float32
BF16 = jnp.bfloat16
VMEM_BYTES = 67043328


def dot(a, b):
    return jnp.dot(a, b, preferred_element_type=F32)


def gram(x):
    return lax.dot_general(x, x, (((0,), (0,)), ((), ())), preferred_element_type=F32)


def halves(x):
    high = x.astype(BF16)
    return high, (x - high.astype(F32)).astype(BF16)


def offset_of(slot, reach):
    return slot - reach if slot < reach else slot - reach + 1


def kernel(
    n_grid, n_band, bounds_hbm, count_hbm, states_hbm, potential_hbm, send_rows_hbm, table_hbm, filtered, margin,
    bounds, count, states, potential, send_rows, table, fetched, table_pad, send_pad, picks, near_hi, near_lo, far_hi, far_lo, out_box, in_box, bands, total,
    share_out, share_in, halo_sent, halo_got, band_sent, band_got, share_sent, share_got,
):
    rows, width = states.shape
    slots, _, halo = send_rows.shape
    reach = slots // 2
    stencil = table.shape[0]
    outer = rows - INNER
    per = margin.shape[0]
    g = lax.axis_index("grid")
    b = lax.axis_index("band")

    fetches = [
        pltpu.make_async_copy(source, place, fetched.at[i])
        for i, (source, place) in enumerate(
            (
                (send_rows_hbm, send_rows),
                (count_hbm, count),
                (states_hbm, states),
                (table_hbm, table),
                (potential_hbm, potential),
                (bounds_hbm, bounds),
            )
        )
    ]
    for fetch in fetches:
        fetch.start()
    in_box[...] = jnp.zeros_like(in_box)
    barrier = pltpu.get_barrier_semaphore()
    for d in range(1, n_grid):
        pl.semaphore_signal(barrier, inc=1, device_id={"grid": lax.rem(g + d, n_grid)}, device_id_type=MESH)
    for d in range(1, n_band):
        pl.semaphore_signal(barrier, inc=1, device_id={"band": lax.rem(b + d, n_band)}, device_id_type=MESH)

    send_pad[...] = jnp.full(send_pad.shape, -1.0, F32)
    fetches[0].wait()
    for k in range(slots):
        send_pad[k : k + 1, :halo] = send_rows[k].astype(F32)
    send_columns = send_pad[...].T
    lanes = lax.broadcasted_iota(jnp.int32, (halo, rows), 1).astype(F32)
    for k in range(slots):
        hit = send_columns[:halo, k : k + 1] == lanes
        picks[k * halo : (k + 1) * halo, :] = jnp.where(hit, 1.0, 0.0).astype(BF16)

    def halo_copy(i, k, target):
        return pltpu.make_async_remote_copy(
            src_ref=out_box.at[i, k],
            dst_ref=in_box.at[i, k],
            send_sem=halo_sent.at[i, k],
            recv_sem=halo_got.at[i, k],
            device_id={"grid": target},
            device_id_type=MESH,
        )

    def send_halo(i, field):
        out_box[i] = dot(picks[...], field.astype(BF16)).astype(BF16).reshape(slots, halo, width)
        if i == 0:
            pl.semaphore_wait(barrier, n_grid - 1 + n_band - 1)
        for k in range(slots):
            target = g + offset_of(k, reach)

            @pl.when(jnp.logical_and(target >= 0, target < n_grid))
            def _():
                halo_copy(i, k, target).start()

    def wait_halo(i):
        for k in range(slots):
            source = g - offset_of(k, reach)

            @pl.when(jnp.logical_and(source >= 0, source < n_grid))
            def _():
                halo_copy(i, k, g).wait_recv()

    fetches[1].wait()
    fetches[2].wait()
    live = lax.broadcasted_iota(jnp.int32, (rows, width), 0) < count[...]
    previous = jnp.zeros((rows, width), F32)
    current = jnp.where(live, states[...], 0.0)
    send_halo(0, current)

    fetches[3].wait()
    fetches[4].wait()
    table_pad[...] = jnp.zeros_like(table_pad)
    table_pad[:stencil, :] = table[...].astype(F32)
    table_pad[stencil : stencil + 1, :] = potential[...]
    columns = table_pad[...].T
    weights = [-KINETIC_SCALE * DIFFERENCE_WEIGHTS[s % SPAN + 1] for s in range(stencil)]

    def weigh(first, size, start, extent):
        ids = (lax.broadcasted_iota(jnp.int32, (size, extent), 1) + start).astype(F32)
        acc = jnp.zeros((size, extent), F32)
        for s in range(stencil):
            acc = acc + jnp.where(columns[first : first + size, s : s + 1] == ids, weights[s], 0.0)
        return halves(acc)

    chunk = 32
    for first in range(0, rows, chunk):
        near_hi[first : first + chunk, :], near_lo[first : first + chunk, :] = weigh(first, chunk, 0, rows)
    for first in range(INNER, rows, chunk):
        at = slice(first - INNER, first - INNER + chunk)
        far_hi[at, :], far_lo[at, :] = weigh(first, chunk, rows + 1, slots * halo)

    fetches[5].wait()
    lower, cutoff, upper = (jnp.broadcast_to(bounds[:, j : j + 1], (8, width)) for j in range(3))
    half_width = (upper - cutoff) / 2.0
    middle = (upper + cutoff) / 2.0
    sigma = half_width / (lower - middle)
    twice_inverse = 2.0 / sigma
    diagonal = columns[:, stencil : stencil + 1] + CENTRE_WEIGHT - middle[:1, :]

    def near(field):
        high, low = halves(field)
        a = near_hi[...]
        return diagonal * field + (dot(a, high) + (dot(a, low) + dot(near_lo[...], high)))

    def far(i):
        box = in_box[i].reshape(slots * halo, width)
        return dot(far_hi[...], box) + dot(far_lo[...], box)

    gain = sigma / half_width
    back = jnp.zeros_like(sigma)
    for i in range(DEGREE):
        own = near(current)
        base = own * gain[:1, :] - back[:1, :] * previous
        if i < DEGREE - 1:
            wait_halo(i)
            outer_rows = base[INNER:] + far(i) * gain[:1, :]
            previous, current = current, jnp.concatenate([base[:INNER], outer_rows], axis=0)
            send_halo(i + 1, current)
            sigma_next = 1.0 / (twice_inverse - sigma)
            gain = 2.0 * sigma_next / half_width
            back = sigma * sigma_next
            sigma = sigma_next

    def band_copy(part, d):
        at = pl.ds(0, INNER) if part == 0 else pl.ds(INNER, outer)
        place = bands.at[b, at]
        return pltpu.make_async_remote_copy(
            src_ref=place,
            dst_ref=place,
            send_sem=band_sent.at[part, d - 1],
            recv_sem=band_got.at[part, d - 1],
            device_id={"band": lax.rem(b + d, n_band)},
            device_id_type=MESH,
        )

    def every_band(at):
        return jnp.concatenate([bands[j, at, :] for j in range(n_band)], axis=1)

    top, bottom = slice(0, INNER), slice(INNER, rows)
    filtered[top, :] = base[top]
    bands[b, top, :] = base[top].astype(BF16)
    for d in range(1, n_band):
        band_copy(0, d).start()
    wait_halo(DEGREE - 1)
    last = base[bottom] + far(DEGREE - 1) * gain[:1, :]
    bands[b, bottom, :] = last.astype(BF16)
    for d in range(1, n_band):
        band_copy(1, d).start()
    filtered[bottom, :] = last
    for d in range(1, n_band):
        band_copy(0, d).wait_recv()
    total[...] = gram(every_band(top))
    for d in range(1, n_band):
        band_copy(1, d).wait_recv()
    total[...] += gram(every_band(bottom))

    def share_copy(d):
        return pltpu.make_async_remote_copy(
            src_ref=share_out.at[d - 1],
            dst_ref=share_in.at[d - 1],
            send_sem=share_sent.at[d - 1],
            recv_sem=share_got.at[d - 1],
            device_id={"grid": lax.rem(g + d, n_grid)},
            device_id_type=MESH,
        )

    def share_of(owner):
        if per % 8 == 0:
            return total[pl.ds(pl.multiple_of((owner * n_band + b) * per, per), per), :]
        group = total[pl.ds(pl.multiple_of(owner * n_band * per, n_band * per), n_band * per), :]
        chosen = group[:per]
        for j in range(1, n_band):
            chosen = jnp.where(b == j, group[j * per : (j + 1) * per], chosen)
        return chosen

    for d in range(1, n_grid):
        share_out[d - 1] = share_of(lax.rem(g + d, n_grid)).astype(BF16)
    for d in range(1, n_grid):
        share_copy(d).start()
    result = share_of(g)
    for d in range(1, n_grid):
        share_copy(d).wait_recv()
    for d in range(1, n_grid):
        result = result + share_in[d - 1].astype(F32)
    margin[...] = result * (1.0 / (n_grid * rows))

    for i in range(DEGREE):
        for k in range(slots):
            target = g + offset_of(k, reach)

            @pl.when(jnp.logical_and(target >= 0, target < n_grid))
            def _():
                halo_copy(i, k, target).wait_send()

    for d in range(1, n_band):
        band_copy(0, d).wait_send()
        band_copy(1, d).wait_send()
    for d in range(1, n_grid):
        share_copy(d).wait_send()


def finish(filtered, margin, filtered_out, margin_out, sems):
    copies = [
        pltpu.make_async_copy(filtered, filtered_out, sems.at[0]),
        pltpu.make_async_copy(margin, margin_out, sems.at[1]),
    ]
    for copy in copies:
        copy.start()
    for copy in copies:
        copy.wait()


def on_device(n_grid, n_band, states, potential, bounds, point_count, send_rows, stencil_table):
    rows, width = states.shape
    slots, halo = send_rows.shape[1:]
    i32 = jnp.int32
    total_bands = width * n_band
    per = total_bands // (n_grid * n_band)
    vmem = pl.BlockSpec(memory_space=pltpu.VMEM)
    hbm = pl.BlockSpec(memory_space=pl.ANY)
    dma = pltpu.SemaphoreType.DMA
    outs = (
        jax.ShapeDtypeStruct((rows, width), F32),
        jax.ShapeDtypeStruct((per, total_bands), F32),
    )
    made = pl.pallas_call(
        functools.partial(kernel, n_grid, n_band),
        out_shape=tuple(pltpu.VMEM(out.shape, out.dtype) for out in outs),
        in_specs=[pl.BlockSpec(memory_space=pltpu.HBM)] * 6,
        out_specs=(vmem, vmem),
        scratch_shapes=[
            pltpu.VMEM((1, 3), F32),
            pltpu.VMEM((1, 1), i32),
            pltpu.VMEM((rows, width), F32),
            pltpu.VMEM((1, rows), F32),
            pltpu.VMEM((slots, 1, halo), i32),
            pltpu.VMEM(stencil_table.shape, i32),
            dma((6,)),
            pltpu.VMEM((128, rows), F32),
            pltpu.VMEM((128, 128), F32),
            pltpu.VMEM((slots * halo, rows), BF16),
            pltpu.VMEM((rows, rows), BF16),
            pltpu.VMEM((rows, rows), BF16),
            pltpu.VMEM((rows - INNER, slots * halo), BF16),
            pltpu.VMEM((rows - INNER, slots * halo), BF16),
            pltpu.VMEM((DEGREE, slots, halo, width), BF16),
            pltpu.VMEM((DEGREE, slots, halo, width), BF16),
            pltpu.VMEM((n_band, rows, width), BF16),
            pltpu.VMEM((total_bands, total_bands), F32),
            pltpu.VMEM((n_grid - 1, per, total_bands), BF16),
            pltpu.VMEM((n_grid - 1, per, total_bands), BF16),
            dma((DEGREE, slots)),
            dma((DEGREE, slots)),
            dma((2, n_band - 1)),
            dma((2, n_band - 1)),
            dma((n_grid - 1,)),
            dma((n_grid - 1,)),
        ],
        compiler_params=pltpu.CompilerParams(
            collective_id=0, has_side_effects=True, vmem_limit_bytes=VMEM_BYTES - 8 * (rows * width + per * total_bands)
        ),
    )(
        bounds.reshape(1, 3),
        point_count.reshape(1, 1),
        states,
        potential.reshape(1, rows),
        jnp.transpose(send_rows, (1, 0, 2)),
        stencil_table,
    )
    return pl.pallas_call(
        finish,
        out_shape=outs,
        in_specs=[vmem, vmem],
        out_specs=(hbm, hbm),
        scratch_shapes=[dma((2,))],
        compiler_params=pltpu.CompilerParams(vmem_limit_bytes=24 * 1024 * 1024),
    )(*made)


def solution(mesh):
    placed = (P("grid", "band"), P("grid"), P(), P("grid"), P("grid", None, None), P(None, "grid"))
    return jax.shard_map(
        functools.partial(on_device, mesh.shape["grid"], mesh.shape["band"]),
        mesh=mesh,
        in_specs=placed,
        out_specs=(P("grid", "band"), P(("grid", "band"), None)),
        check_vma=False,
    )
```

```python
import functools

import jax
import jax.numpy as jnp
from jax import lax
from jax.experimental import pallas as pl
from jax.experimental.pallas import tpu as pltpu
from jax.sharding import PartitionSpec as P

SPAN = 6
DEGREE = 3
INNER = 160

DIFFERENCE_WEIGHTS = (
    -5369.0 / 1800.0,
    12.0 / 7.0,
    -15.0 / 56.0,
    10.0 / 189.0,
    -1.0 / 112.0,
    2.0 / 1925.0,
    -1.0 / 16632.0,
)
KINETIC_SCALE = 0.5 / 0.49
CENTRE_WEIGHT = -3.0 * KINETIC_SCALE * DIFFERENCE_WEIGHTS[0]

MESH = pl.DeviceIdType.MESH
F32 = jnp.float32
BF16 = jnp.bfloat16
VMEM_BYTES = 67043328


def dot(a, b):
    return jnp.dot(a, b, preferred_element_type=F32)


def gram(x):
    return lax.dot_general(x, x, (((0,), (0,)), ((), ())), preferred_element_type=F32)


def halves(x):
    high = x.astype(BF16)
    return high, (x - high.astype(F32)).astype(BF16)


def offset_of(slot, reach):
    return slot - reach if slot < reach else slot - reach + 1


def kernel(
    n_grid, n_band, bounds_hbm, count_hbm, states_hbm, potential_hbm, send_rows_hbm, table_hbm, filtered, margin,
    bounds, count, states, potential, send_rows, table, fetched, table_pad, send_pad, picks, near_hi, near_lo, far_hi, far_lo, out_box, in_box, bands, total,
    share_out, share_in, greetings, passed_hi, passed_lo, halo_sent, halo_got, band_sent, band_got, share_sent, share_got,
):
    rows, width = states.shape
    slots, _, halo = send_rows.shape
    reach = slots // 2
    stencil = table.shape[0]
    outer = rows - INNER
    per = margin.shape[0]
    g = lax.axis_index("grid")
    b = lax.axis_index("band")
    side = lax.rem(g // 2, 2)

    fetches = [
        pltpu.make_async_copy(source, place, fetched.at[i])
        for i, (source, place) in enumerate(
            (
                (send_rows_hbm, send_rows),
                (count_hbm, count),
                (states_hbm, states),
                (table_hbm, table),
                (potential_hbm, potential),
                (bounds_hbm, bounds),
            )
        )
    ]
    for fetch in fetches:
        fetch.start()
    in_box[...] = jnp.zeros_like(in_box)
    barrier = pltpu.get_barrier_semaphore()
    def at_distance(distance, act):
        for target in (g - distance, g + distance):

            @pl.when(jnp.logical_and(target >= 0, target < n_grid))
            def _():
                act(target)

    def greet(semaphore, first, final):
        for distance in range(first, final + 1):
            at_distance(
                distance,
                lambda target: pl.semaphore_signal(
                    semaphore, inc=1, device_id={"grid": target}, device_id_type=MESH
                ),
            )

    def peers(first, final):
        number = 0
        for distance in range(first, final + 1):
            for target in (g - distance, g + distance):
                number = number + jnp.where(jnp.logical_and(target >= 0, target < n_grid), 1, 0)
        return number

    def greeted(semaphore, first, final):
        pl.semaphore_wait(semaphore, peers(first, final))

    greet(barrier, 1, min(reach, n_grid - 1))
    for d in range(1, n_band):
        pl.semaphore_signal(barrier, inc=1, device_id={"band": lax.rem(b + d, n_band)}, device_id_type=MESH)

    send_pad[...] = jnp.full(send_pad.shape, -1.0, F32)
    fetches[0].wait()
    for k in range(slots):
        send_pad[k : k + 1, :halo] = send_rows[k].astype(F32)
    send_columns = send_pad[...].T
    lanes = lax.broadcasted_iota(jnp.int32, (halo, rows), 1).astype(F32)
    for k in range(slots):
        hit = send_columns[:halo, k : k + 1] == lanes
        picks[k * halo : (k + 1) * halo, :] = jnp.where(hit, 1.0, 0.0).astype(BF16)

    def halo_copy(i, k, target):
        return pltpu.make_async_remote_copy(
            src_ref=out_box.at[i, k],
            dst_ref=in_box.at[i, k],
            send_sem=halo_sent.at[i, k],
            recv_sem=halo_got.at[i, k],
            device_id={"grid": target},
            device_id_type=MESH,
        )

    def send_halo(i, chosen):
        out_box[i] = chosen.astype(BF16).reshape(slots, halo, width)
        if i == 0:
            pl.semaphore_wait(barrier, n_band - 1 + peers(1, min(reach, n_grid - 1)))
        for order in range(slots):
            k = jnp.where(side == 0, order, slots - 1 - order)
            target = g + k - reach + jnp.where(k < reach, 0, 1)

            @pl.when(jnp.logical_and(target >= 0, target < n_grid))
            def _():
                halo_copy(i, k, target).start()

    def wait_halo(i):
        for k in range(slots):
            source = g - offset_of(k, reach)

            @pl.when(jnp.logical_and(source >= 0, source < n_grid))
            def _():
                halo_copy(i, k, g).wait_recv()

    fetches[1].wait()
    fetches[2].wait()
    live = lax.broadcasted_iota(jnp.int32, (rows, width), 0) < count[...]
    previous = jnp.zeros((rows, width), F32)
    current = jnp.where(live, states[...], 0.0)
    send_halo(0, dot(picks[...], current.astype(BF16)))

    fetches[3].wait()
    fetches[4].wait()
    table_pad[...] = jnp.zeros_like(table_pad)
    table_pad[:stencil, :] = table[...].astype(F32)
    table_pad[stencil : stencil + 1, :] = potential[...]
    columns = table_pad[...].T
    weights = [-KINETIC_SCALE * DIFFERENCE_WEIGHTS[s % SPAN + 1] for s in range(stencil)]

    def weigh(first, size, start, extent):
        pieces = []
        for begin in range(0, extent, 256):
            wide = min(256, extent - begin)
            ids = lax.broadcasted_iota(jnp.int32, (size, wide), 1).astype(F32).astype(BF16)
            rows_of = (columns[first : first + size, :stencil] - float(start + begin)).astype(BF16)
            one, none = jnp.ones((size, wide), BF16), jnp.zeros((size, wide), BF16)
            acc = jnp.zeros((size, wide), F32)
            for j in range(SPAN):
                tally = none
                for s in range(j, stencil, SPAN):
                    tally = tally + jnp.where(rows_of[:, s : s + 1] == ids, one, none)
                acc = acc + weights[j] * tally.astype(F32)
            pieces.append(acc)
        return halves(jnp.concatenate(pieces, axis=1))

    chunk = 32
    for first in range(0, rows, chunk):
        near_hi[first : first + chunk, :], near_lo[first : first + chunk, :] = weigh(first, chunk, 0, rows)
    for first in range(INNER, rows, chunk):
        at = slice(first - INNER, first - INNER + chunk)
        far_hi[at, :], far_lo[at, :] = weigh(first, chunk, rows + 1, slots * halo)
    passed_hi[...] = dot(picks[:, INNER:], far_hi[...]).astype(BF16)
    passed_lo[...] = dot(picks[:, INNER:], far_lo[...]).astype(BF16)

    fetches[5].wait()
    lower, cutoff, upper = (jnp.broadcast_to(bounds[:, j : j + 1], (8, width)) for j in range(3))
    half_width = (upper - cutoff) / 2.0
    middle = (upper + cutoff) / 2.0
    sigma = half_width / (lower - middle)
    twice_inverse = 2.0 / sigma
    diagonal = columns[:, stencil : stencil + 1] + CENTRE_WEIGHT - middle[:1, :]

    def near(field):
        high, low = halves(field)
        a = near_hi[...]
        return diagonal * field + (dot(a, high) + (dot(a, low) + dot(near_lo[...], high)))

    def far(i):
        box = in_box[i].reshape(slots * halo, width)
        return dot(far_hi[...], box) + dot(far_lo[...], box)

    gain = sigma / half_width
    back = jnp.zeros_like(sigma)
    for i in range(DEGREE):
        own = near(current)
        base = own * gain[:1, :] - back[:1, :] * previous
        if i < DEGREE - 1:
            high, low = halves(base)
            chosen = dot(picks[...], high) + dot(picks[...], low)
            if i == 1:
                greeted(greetings.at[0], reach + 1, min(2 * reach, n_grid - 1))
            wait_halo(i)
            box = in_box[i].reshape(slots * halo, width)
            passed = dot(passed_hi[...], box) + dot(passed_lo[...], box)
            send_halo(i + 1, chosen + passed * gain[:1, :])
            outer_rows = base[INNER:] + far(i) * gain[:1, :]
            previous, current = current, jnp.concatenate([base[:INNER], outer_rows], axis=0)
            if i == 0:
                greet(greetings.at[0], reach + 1, min(2 * reach, n_grid - 1))
            sigma_next = 1.0 / (twice_inverse - sigma)
            gain = 2.0 * sigma_next / half_width
            back = sigma * sigma_next
            sigma = sigma_next

    def band_copy(part, d):
        at = pl.ds(0, INNER) if part == 0 else pl.ds(INNER, outer)
        place = bands.at[b, at]
        return pltpu.make_async_remote_copy(
            src_ref=place,
            dst_ref=place,
            send_sem=band_sent.at[part, d - 1],
            recv_sem=band_got.at[part, d - 1],
            device_id={"band": lax.rem(b + d, n_band)},
            device_id_type=MESH,
        )

    def every_band(at):
        return jnp.concatenate([bands[j, at, :] for j in range(n_band)], axis=1)

    top, bottom = slice(0, INNER), slice(INNER, rows)
    filtered[top, :] = base[top]
    bands[b, top, :] = base[top].astype(BF16)
    for d in range(1, n_band):
        band_copy(0, d).start()
    wait_halo(DEGREE - 1)
    last = base[bottom] + far(DEGREE - 1) * gain[:1, :]
    bands[b, bottom, :] = last.astype(BF16)
    for d in range(1, n_band):
        band_copy(1, d).start()
    filtered[bottom, :] = last
    for d in range(1, n_band):
        band_copy(0, d).wait_recv()
    total[...] = gram(every_band(top))
    for d in range(1, n_band):
        band_copy(1, d).wait_recv()
    total[...] += gram(every_band(bottom))

    def share_copy(d):
        return pltpu.make_async_remote_copy(
            src_ref=share_out.at[d - 1],
            dst_ref=share_in.at[d - 1],
            send_sem=share_sent.at[d - 1],
            recv_sem=share_got.at[d - 1],
            device_id={"grid": lax.rem(g + d, n_grid)},
            device_id_type=MESH,
        )

    def share_of(owner):
        if per % 8 == 0:
            return total[pl.ds(pl.multiple_of((owner * n_band + b) * per, per), per), :]
        group = total[pl.ds(pl.multiple_of(owner * n_band * per, n_band * per), n_band * per), :]
        chosen = group[:per]
        for j in range(1, n_band):
            chosen = jnp.where(b == j, group[j * per : (j + 1) * per], chosen)
        return chosen

    for d in range(1, n_grid):
        share_out[d - 1] = share_of(lax.rem(g + d, n_grid)).astype(BF16)
    heard, known, turn = 2 * reach, 5 * reach, 1
    while known < n_grid - 1:
        final = min(known, n_grid - 1)
        greet(greetings.at[turn], heard + 1, final)
        greeted(greetings.at[turn], heard + 1, final)
        heard, known, turn = known, 2 * known, turn + 1
    upper_half = 2 * g >= n_grid
    for order in range(n_grid - 1):
        other = jnp.where(upper_half, order, n_grid - 1 - order)
        skip = jnp.where(upper_half, jnp.where(other >= g, 1, 0), jnp.where(other <= g, -1, 0))
        share_copy(lax.rem(other + skip - g + n_grid, n_grid)).start()
    result = share_of(g)
    for d in range(1, n_grid):
        share_copy(d).wait_recv()
    for d in range(1, n_grid):
        result = result + share_in[d - 1].astype(F32)
    margin[...] = result * (1.0 / (n_grid * rows))

    for i in range(DEGREE):
        for k in range(slots):
            target = g + offset_of(k, reach)

            @pl.when(jnp.logical_and(target >= 0, target < n_grid))
            def _():
                halo_copy(i, k, target).wait_send()

    for d in range(1, n_band):
        band_copy(0, d).wait_send()
        band_copy(1, d).wait_send()
    for d in range(1, n_grid):
        share_copy(d).wait_send()


def finish(filtered, margin, filtered_out, margin_out, sems):
    copies = [
        pltpu.make_async_copy(filtered, filtered_out, sems.at[0]),
        pltpu.make_async_copy(margin, margin_out, sems.at[1]),
    ]
    for copy in copies:
        copy.start()
    for copy in copies:
        copy.wait()


def on_device(n_grid, n_band, states, potential, bounds, point_count, send_rows, stencil_table):
    rows, width = states.shape
    slots, halo = send_rows.shape[1:]
    i32 = jnp.int32
    total_bands = width * n_band
    per = total_bands // (n_grid * n_band)
    vmem = pl.BlockSpec(memory_space=pltpu.VMEM)
    hbm = pl.BlockSpec(memory_space=pl.ANY)
    dma = pltpu.SemaphoreType.DMA
    outs = (
        jax.ShapeDtypeStruct((rows, width), F32),
        jax.ShapeDtypeStruct((per, total_bands), F32),
    )
    made = pl.pallas_call(
        functools.partial(kernel, n_grid, n_band),
        out_shape=tuple(pltpu.VMEM(out.shape, out.dtype) for out in outs),
        in_specs=[pl.BlockSpec(memory_space=pltpu.HBM)] * 6,
        out_specs=(vmem, vmem),
        scratch_shapes=[
            pltpu.VMEM((1, 3), F32),
            pltpu.VMEM((1, 1), i32),
            pltpu.VMEM((rows, width), F32),
            pltpu.VMEM((1, rows), F32),
            pltpu.VMEM((slots, 1, halo), i32),
            pltpu.VMEM(stencil_table.shape, i32),
            dma((6,)),
            pltpu.VMEM((128, rows), F32),
            pltpu.VMEM((128, 128), F32),
            pltpu.VMEM((slots * halo, rows), BF16),
            pltpu.VMEM((rows, rows), BF16),
            pltpu.VMEM((rows, rows), BF16),
            pltpu.VMEM((rows - INNER, slots * halo), BF16),
            pltpu.VMEM((rows - INNER, slots * halo), BF16),
            pltpu.VMEM((DEGREE, slots, halo, width), BF16),
            pltpu.VMEM((DEGREE, slots, halo, width), BF16),
            pltpu.VMEM((n_band, rows, width), BF16),
            pltpu.VMEM((total_bands, total_bands), F32),
            pltpu.VMEM((n_grid - 1, per, total_bands), BF16),
            pltpu.VMEM((n_grid - 1, per, total_bands), BF16),
            pltpu.SemaphoreType.REGULAR((n_grid,)),
            pltpu.VMEM((slots * halo, slots * halo), BF16),
            pltpu.VMEM((slots * halo, slots * halo), BF16),
            dma((DEGREE, slots)),
            dma((DEGREE, slots)),
            dma((2, n_band - 1)),
            dma((2, n_band - 1)),
            dma((n_grid - 1,)),
            dma((n_grid - 1,)),
        ],
        compiler_params=pltpu.CompilerParams(
            collective_id=0, has_side_effects=True, vmem_limit_bytes=VMEM_BYTES - 8 * (rows * width + per * total_bands)
        ),
    )(
        bounds.reshape(1, 3),
        point_count.reshape(1, 1),
        states,
        potential.reshape(1, rows),
        jnp.transpose(send_rows, (1, 0, 2)),
        stencil_table,
    )
    return pl.pallas_call(
        finish,
        out_shape=outs,
        in_specs=[vmem, vmem],
        out_specs=(hbm, hbm),
        scratch_shapes=[dma((2,))],
        compiler_params=pltpu.CompilerParams(vmem_limit_bytes=24 * 1024 * 1024),
    )(*made)


def solution(mesh):
    placed = (P("grid", "band"), P("grid"), P(), P("grid"), P("grid", None, None), P(None, "grid"))
    return jax.shard_map(
        functools.partial(on_device, mesh.shape["grid"], mesh.shape["band"]),
        mesh=mesh,
        in_specs=placed,
        out_specs=(P("grid", "band"), P(("grid", "band"), None)),
        check_vma=False,
    )
```
